32 devices in a mesh: grp: 2 (over x), dev: 16 (over z, y, core).
Axes of the slice: x: 2, y: 2, z: 4, core: 2. Of those that a mesh axis runs over, the one named last changes fastest.
Arguments:
- voltages: int32 [512, 137216], P('dev', 'grp'), may hold values from -2147483648 to 2147483646
- block_order: int32 [10], replicated, may hold values from 0 to 9, each once
Outputs:
- visibilities: float32 [10, 2, 2, 1024, 128, 128], P('grp', None, None, 'dev')
The draws below stay inside these ranges and needn't reach their ends.
Inputs may be any that keep to these rules, and one draw needn't show every extreme that they name: `block_order`: a permutation of the block pair numbers.
All inputs are finite; a program needn't handle non-finite values.
Results may differ from the reference program's by a relative error of at most 0.0058.
Values may be sent and summed in bfloat16 or wider, within the bound.
No kernel may reach another device: no remote copies, remote signals or barrier semaphores. Data moves between devices by JAX's collectives and lax.ppermute only.
A program may use at most 320 MiB of HBM per device.

```python
import jax
import jax.numpy as jnp
import numpy as np
from jax import lax

A = 512
FREQ_CHANNELS = 1024
FILTER_TAPS = 4
BLOCK_FRAMES = 64
INTEG_PERIODS = 2
BLOCK = 128
NBP = 10
SBLK = 137216
N_GRP = 2


def touch_ends(drawn, stream_key, smallest, high):
    longest = drawn.shape.index(max(drawn.shape))
    spots = []
    for shift in (0, 1):
        where = [jax.random.randint(jax.random.fold_in(stream_key, axis), (), 0, length) for axis, length in enumerate(drawn.shape)]
        where[longest] = (where[longest] + shift) % drawn.shape[longest]
        spots.append(tuple(where))
    return drawn.at[spots[0]].set(smallest).at[spots[1]].set(high)


def setup_inputs(seed: int = 0) -> dict:
    arg_keys = jax.random.split(jax.random.key(seed), 3)
    return {
        "voltages": touch_ends(jax.random.randint(arg_keys[0], (A, N_GRP * INTEG_PERIODS * SBLK // 4), -2147483648, 2147483647), jax.random.fold_in(arg_keys[0], 1), -2147483648, 2147483646).astype(jnp.int32),
        "block_order": jax.random.permutation(arg_keys[1], NBP).astype(jnp.int32),
    }


def unpack_packed_words(words):
    pieces = []
    for byte in range(4):
        raw = jnp.bitwise_and(jnp.right_shift(words, 8 * byte), 255)
        pieces.append((raw - 128).astype(jnp.float32) / 64.0)
    return jnp.concatenate(pieces, axis=-1)


def prototype():
    length = 2 * FREQ_CHANNELS
    position = jnp.arange(FILTER_TAPS * length, dtype=jnp.float32) + 0.5
    window = 0.5 - 0.5 * jnp.cos(2.0 * jnp.pi * position / (length * FILTER_TAPS))
    return jnp.sinc(position / length - FILTER_TAPS / 2.0) * window


def dft_table():
    length = 2 * FREQ_CHANNELS
    index = jnp.arange(length, dtype=jnp.int32)[:, None] * jnp.arange(FREQ_CHANNELS, dtype=jnp.int32)[None, :]
    angle = (2.0 * jnp.pi / length) * (index % length).astype(jnp.float32)
    factor = length ** -0.5
    return jnp.stack([jnp.cos(angle) * factor, -jnp.sin(angle) * factor], axis=1).astype(jnp.bfloat16)


def filter_frames(voltage_samples, coeffs):
    weights = coeffs.reshape(FILTER_TAPS, 2 * FREQ_CHANNELS)
    total = voltage_samples[..., 0:BLOCK_FRAMES, :] * weights[0]
    for shift in range(1, FILTER_TAPS):
        total = total + voltage_samples[..., shift:shift + BLOCK_FRAMES, :] * weights[shift]
    return total.astype(jnp.bfloat16)


def pick(table, index):
    hits = jnp.arange(table.shape[0], dtype=jnp.int32) == index
    return jnp.sum(jnp.where(hits, table, 0)).astype(jnp.int32)


def block_gram(data, slots, block_order, factor):
    twisted = jnp.stack([data[..., 1, :], -data[..., 0, :]], axis=-2)
    upper_rows, upper_cols = np.triu_indices(A // BLOCK)
    pair_rows = jnp.asarray(upper_rows.astype(np.int32))
    pair_cols = jnp.asarray(upper_cols.astype(np.int32))

    def one_slot(slot):
        entry = pick(block_order, slot)
        row = pick(pair_rows, entry) * BLOCK
        col = pick(pair_cols, entry) * BLOCK
        left = lax.dynamic_slice_in_dim(data, row, BLOCK, 1).astype(jnp.float32)
        left_twist = lax.dynamic_slice_in_dim(twisted, row, BLOCK, 1).astype(jnp.float32)
        right = lax.dynamic_slice_in_dim(data, col, BLOCK, 1).astype(jnp.float32)
        real = jnp.einsum('cagirf,cbgirf->icab', left, right)
        imag = jnp.einsum('cagirf,cbgirf->icab', left_twist, right)
        return jnp.stack([real, imag], axis=1) * factor

    return lax.map(one_slot, slots)


def reference(voltages, block_order):
    coeffs = prototype()
    table = dft_table().astype(jnp.float32)
    words = voltages.reshape(A, N_GRP, INTEG_PERIODS, -1)
    groups = []
    for group in range(N_GRP):
        integrations = []
        for integ in range(INTEG_PERIODS):
            voltage_samples = unpack_packed_words(words[:, group, integ]).reshape(A, BLOCK_FRAMES + FILTER_TAPS - 1, 2 * FREQ_CHANNELS)
            filtered = filter_frames(voltage_samples, coeffs)
            channel_spectra = jnp.einsum('afn,nrc->carf', filtered.astype(jnp.float32), table)
            integrations.append(channel_spectra.astype(jnp.bfloat16))
        groups.append(jnp.stack(integrations, axis=2))
    data = jnp.stack(groups, axis=2)
    slots = jnp.arange(NBP, dtype=jnp.int32)
    return block_gram(data, slots, block_order, 1.0 / (N_GRP * BLOCK_FRAMES))
```

```python
import functools

import jax
import jax.numpy as jnp
import numpy as np
from jax import lax
from jax.experimental import pallas as pl
from jax.experimental.pallas import tpu as pltpu
from jax.sharding import PartitionSpec as P

FREQ_CHANNELS = 1024
FILTER_TAPS = 4
BLOCK_FRAMES = 64
INTEG_PERIODS = 2
BLOCK = 128
LENGTH = 2 * FREQ_CHANNELS
QUARTER = LENGTH // 4
WORD_ROWS = BLOCK_FRAMES + FILTER_TAPS - 1
QUAD = 4
CHUNKS = 4


def prototype():
    position = jnp.arange(FILTER_TAPS * LENGTH, dtype=jnp.float32) + 0.5
    window = 0.5 - 0.5 * jnp.cos(2.0 * jnp.pi * position / (LENGTH * FILTER_TAPS))
    return jnp.sinc(position / LENGTH - FILTER_TAPS / 2.0) * window


def dft_rows(devices, chunks):
    channels = jnp.arange(FREQ_CHANNELS, dtype=jnp.int32)
    channels = channels.reshape(devices, chunks, -1).swapaxes(0, 1).reshape(-1)
    index = channels[:, None] * jnp.arange(LENGTH, dtype=jnp.int32)[None, :]
    angle = 2.0 * jnp.pi / LENGTH * (index % LENGTH).astype(jnp.float32)
    factor = LENGTH ** (-0.5)
    return jnp.stack([jnp.cos(angle) * factor, -jnp.sin(angle) * factor]).astype(jnp.bfloat16)


def spectra_kernel(words_ref, weights_ref, table_ref, *refs, group, chunks):
    outs = refs[:chunks]
    planes, filtered, scratch = refs[chunks:]
    for quad in range(group // QUAD):
        for part in range(QUAD):
            antenna = quad * QUAD + part
            for lane in range(QUARTER // 128):
                words = words_ref[antenna, 0, :, lane * 128 : (lane + 1) * 128]
                flipped = words ^ jnp.int32(-2139062144)
                for byte in range(4):
                    value = lax.shift_right_arithmetic(flipped << (24 - 8 * byte), 24)
                    planes[lane, byte * WORD_ROWS : (byte + 1) * WORD_ROWS, :] = value.astype(jnp.float32)
            for lane in range(QUARTER // 128):
                for m in range(4):
                    start = m * QUARTER + lane * 128
                    total = None
                    for tap in range(FILTER_TAPS):
                        piece = planes[lane, pl.ds(4 * tap + m, BLOCK_FRAMES, stride=4), :]
                        term = piece * weights_ref[tap : tap + 1, start : start + 128]
                        total = term if total is None else total + term
                    filtered[part * BLOCK_FRAMES : (part + 1) * BLOCK_FRAMES, start : start + 128] = total.astype(
                        jnp.bfloat16
                    )
        frames = filtered[...]
        rows = FREQ_CHANNELS // chunks
        low = lax.broadcasted_iota(jnp.int32, (rows, 128), 1) < BLOCK_FRAMES
        for chunk in range(chunks):
            both = []
            for r in range(2):
                both.append(
                    lax.dot_general(
                        table_ref[r, chunk * rows : (chunk + 1) * rows, :],
                        frames,
                        (((1,), (1,)), ((), ())),
                        preferred_element_type=jnp.float32,
                    )
                )
            for pair in range(QUAD // 2):
                real = both[0][:, pair * 128 : (pair + 1) * 128]
                imag = both[1][:, pair * 128 : (pair + 1) * 128]
                first = jnp.where(low, real, pltpu.roll(imag, 64, 1))
                second = jnp.where(low, pltpu.roll(real, 64, 1), imag)
                antenna = quad * QUAD + pair * 2
                base = chunk * rows * group
                scratch[pl.ds(base + antenna, rows, stride=group), :] = first
                scratch[pl.ds(base + antenna + 1, rows, stride=group), :] = second
    rows = FREQ_CHANNELS // chunks
    for chunk in range(chunks):
        piece = scratch[chunk * rows * group : (chunk + 1) * rows * group, :]
        outs[chunk][...] = piece.reshape(rows, group, 128).astype(jnp.bfloat16)


def make_spectra(words, weights, table, integ, chunks):
    antennas = words.shape[0]
    group = min(antennas, 16)
    rows = FREQ_CHANNELS // chunks
    return pl.pallas_call(
        functools.partial(spectra_kernel, group=group, chunks=chunks),
        grid=(antennas // group,),
        in_specs=[
            pl.BlockSpec((group, 1, WORD_ROWS, QUARTER), lambda s: (s, integ, 0, 0)),
            pl.BlockSpec((FILTER_TAPS, LENGTH), lambda s: (0, 0)),
            pl.BlockSpec((2, FREQ_CHANNELS, LENGTH), lambda s: (0, 0, 0)),
        ],
        out_specs=[pl.BlockSpec((rows, group, 128), lambda s: (0, s, 0)) for _ in range(chunks)],
        out_shape=[jax.ShapeDtypeStruct((rows, antennas, 128), jnp.bfloat16) for _ in range(chunks)],
        scratch_shapes=[
            pltpu.VMEM((QUARTER // 128, 4 * WORD_ROWS, 128), jnp.float32),
            pltpu.VMEM((QUAD * BLOCK_FRAMES, LENGTH), jnp.bfloat16),
            pltpu.VMEM((FREQ_CHANNELS * group, 128), jnp.float32),
        ],
        name=f"spectra_{integ}",
    )(words, weights, table)


def gram_kernel(picks_ref, *refs, sources, per_block, factor, owned, batch, aliased):
    data = refs[:sources]
    out_ref = refs[sources + (1 if aliased else 0)]
    low = lax.broadcasted_iota(jnp.int32, (BLOCK, 128), 1) < BLOCK_FRAMES
    for channel in range(batch):
        for slot in range(owned):
            row = picks_ref[slot]
            col = picks_ref[owned + slot]
            lefts, rights, twists = [], [], []
            for ref in data:
                left = ref[pl.ds(row * per_block, per_block), channel].reshape(BLOCK, 128)
                right = ref[pl.ds(col * per_block, per_block), channel].reshape(BLOCK, 128)
                turned = pltpu.roll(right.astype(jnp.float32), 64, 1)
                twists.append(jnp.where(low, -turned, turned).astype(jnp.bfloat16))
                lefts.append(left)
                rights.append(right)
            left = jnp.concatenate(lefts, axis=1)
            right = jnp.concatenate([jnp.concatenate(rights, axis=1), jnp.concatenate(twists, axis=1)], axis=0)
            both = lax.dot_general(
                left, right, (((1,), (1,)), ((), ())), preferred_element_type=jnp.float32
            ) * factor
            out_ref[slot, 0, 0, channel] = both[:, :BLOCK]
            out_ref[slot, 0, 1, channel] = both[:, BLOCK:]


def gram(picks, data, carry, integ, chunk, shape, factor):
    devices, count, antennas, _ = data[0].shape
    batch = min(count, 4)
    owned = shape[0]
    steps = count // batch
    aliased = carry is not None
    in_specs = [pl.BlockSpec((devices, batch, antennas, 128), lambda s, p: (0, s, 0, 0)) for _ in data]
    operands = [picks, *data]
    if aliased:
        in_specs.append(pl.BlockSpec(memory_space=pl.ANY))
        operands.append(carry)
    return pl.pallas_call(
        functools.partial(
            gram_kernel,
            sources=len(data),
            per_block=BLOCK // antennas,
            factor=factor,
            owned=owned,
            batch=batch,
            aliased=aliased,
        ),
        grid_spec=pltpu.PrefetchScalarGridSpec(
            num_scalar_prefetch=1,
            grid=(steps,),
            in_specs=in_specs,
            out_specs=pl.BlockSpec(
                (owned, 1, 2, batch, BLOCK, BLOCK), lambda s, p: (0, integ, 0, chunk * steps + s, 0, 0)
            ),
        ),
        out_shape=jax.ShapeDtypeStruct(shape, jnp.float32),
        input_output_aliases={len(operands) - 1: 0} if aliased else {},
        name=f"gram_{integ}_{chunk}",
    )(*operands)


def on_device(voltages, block_order):
    antennas = voltages.shape[0]
    groups = lax.axis_size("grp")
    devices = lax.axis_size("dev")
    blocks = antennas * devices // BLOCK
    owned_count = block_order.shape[0] // groups
    local = FREQ_CHANNELS // devices
    chunks = min(CHUNKS, local)
    words = voltages.reshape(antennas, INTEG_PERIODS, WORD_ROWS, QUARTER)
    weights = prototype().reshape(FILTER_TAPS, LENGTH) / 64.0
    table = dft_rows(devices, chunks)

    upper_rows, upper_cols = np.triu_indices(blocks)
    owned = lax.axis_index("grp") * owned_count + jnp.arange(owned_count, dtype=jnp.int32)
    entries = block_order[owned]
    picks = jnp.concatenate(
        [
            jnp.asarray(upper_rows.astype(np.int32))[entries],
            jnp.asarray(upper_cols.astype(np.int32))[entries],
        ]
    )
    factor = 1.0 / (groups * BLOCK_FRAMES)
    shape = (owned_count, INTEG_PERIODS, 2, local, BLOCK, BLOCK)
    pieces = []
    for integ in range(INTEG_PERIODS):
        pieces.extend(make_spectra(words, weights, table, integ, chunks))
    received = []
    for step, piece in enumerate(pieces):
        if step >= 2:
            piece, received[step - 2] = lax.optimization_barrier((piece, received[step - 2]))
        mine = lax.all_to_all(
            piece.reshape(devices, local // chunks, antennas, 128), "dev", split_axis=0, concat_axis=0, tiled=True
        )
        data = [mine]
        for shift in range(1, groups):
            ring = [(g, (g + shift) % groups) for g in range(groups)]
            data.append(lax.ppermute(mine, "grp", ring))
        received.append(data)
    out = None
    for step, data in enumerate(received):
        out = gram(picks, data, out, step // chunks, step % chunks, shape, factor)
    return out


def solution(mesh):
    in_specs = (P("dev", "grp"), P())
    out_specs = P("grp", None, None, "dev", None, None)
    return jax.shard_map(
        on_device, mesh=mesh, in_specs=in_specs, out_specs=out_specs, check_vma=False
    )
```
